32 devices in a mesh: groups: 2 (over x), ctx: 16 (over z, y, core).
Axes of the slice: x: 2, y: 2, z: 4, core: 2. Of those that a mesh axis runs over, the one named last changes fastest.
Arguments:
- queries: bfloat16 [512, 128, 576], P(('groups', 'ctx')), parts along dimension 0, may hold values from -4 to 4
- latent_cache: bfloat16 [32768, 576], P(('groups', 'ctx')), parts along dimension 0, may hold values from -4 to 4
- block_picks: int32 [32, 32], P(('groups', 'ctx')), parts along dimension 0, may hold values from 0 to 255, as said below
- lengths: int32 [512], P(('groups', 'ctx')), parts along dimension 0, may hold values from 8192 to 16384
Outputs:
- latent_out: bfloat16 [512, 128, 512], P(('groups', 'ctx')), parts along dimension 0
The draws below stay inside these ranges and needn't reach their ends.
There are 2 independent parts, one for each index of `groups`. The reference program is written for one: setup_inputs(seed, part) draws one part's arguments, and reference() takes and returns one part's arrays. A program takes and returns all parts, laid end to end along the dimension named above; each array names one. Nothing has to cross between parts.
Inputs may be any that keep to these rules, and one draw needn't show every extreme that they name: `block_picks`: each row names 32 different blocks. At most 4 of a row's blocks lie in one owner's range of 16 consecutive blocks, and every row reaches this with its first 4 entries, which lie in the first half of the context. Over all rows together at most 8 different blocks of one owner's range are named, and some owner reaches this.
All inputs are finite; a program needn't handle non-finite values.
Results may differ from the reference program's by a relative error of at most 0.0035.
Values may be sent and summed in bfloat16 or wider, within the bound.
A program may use at most 128 MiB of HBM per device.

```python
import jax
import jax.numpy as jnp
from jax import lax

H = 128
LAT = 512
BLOCK = 64
TOPK = 32
BLK_DEV = 16
WIDTH = 576
CONTEXT = 16384
QROWS = 256
N_CTX = 16


def draw_latent_cache(key, part):
    seed_cache = jax.random.fold_in(key, 21)
    values = jnp.clip(jax.random.normal(seed_cache, (CONTEXT, WIDTH), jnp.float32), -4.0, 4.0)
    return values.astype(jnp.bfloat16)


def draw_block_picks(key, part):
    capacity = max(1, 2 * TOPK // N_CTX)
    pair_count = N_CTX * capacity
    starting_picks = jax.random.fold_in(key, 41)
    popular_region_seed, extra_credit_seed, noise_perturbation_seed, permutation_seed, split_choice_seed = jax.random.split(starting_picks, 5)
    hot_owner = jax.random.randint(popular_region_seed, (N_CTX,), 0, max(1, N_CTX // 2))
    hot_owner = hot_owner.at[1].set(hot_owner[0])
    owner_preference_lift = jax.random.randint(extra_credit_seed, (N_CTX,), 0, 2) * 4096
    jitter_amount = jax.random.randint(noise_perturbation_seed, (N_CTX, pair_count), 0, 4096)
    pair_index = jnp.arange(pair_count, dtype=jnp.int32)
    every_pair_holder = pair_index // capacity
    required_blocks = (every_pair_holder[None, :] == hot_owner[:, None]).astype(jnp.int32) * 16384
    block_ratings = jitter_amount + owner_preference_lift[every_pair_holder][None, :] + required_blocks
    block_ratings = block_ratings * pair_count + pair_index[None, :]
    _, chosen = lax.top_k(block_ratings, TOPK)
    pair_owner = chosen // capacity
    pair_slot = chosen % capacity
    ranks = jax.random.randint(permutation_seed, (N_CTX, BLK_DEV), 0, 65536) * BLK_DEV + jnp.arange(BLK_DEV, dtype=jnp.int32)[None, :]
    candidates = jnp.argsort(ranks, axis=1)[:, :2 * capacity].astype(jnp.int32)
    side_bit = jax.random.randint(split_choice_seed, (N_CTX, TOPK), 0, 2)
    group_index = jnp.arange(N_CTX, dtype=jnp.int32)[:, None]
    at_shared = pair_owner == hot_owner[0]
    side_bit = jnp.where((group_index == 0) & at_shared, 0, side_bit)
    side_bit = jnp.where((group_index == 1) & at_shared, 1, side_bit)
    local_block = candidates[pair_owner, 2 * pair_slot + side_bit]
    return (pair_owner * BLK_DEV + local_block).astype(jnp.int32)


def draw_queries(key, part):
    seed_rows = jax.random.fold_in(key, 31)
    array_shape = (QROWS, H, WIDTH)
    values = jnp.clip(jax.random.normal(seed_rows, array_shape, jnp.float32), -4.0, 4.0)
    return values.astype(jnp.bfloat16)


def plant(values, key, least, top_value):
    extent = values.shape
    spot = [jax.random.randint(jax.random.fold_in(key, axis), (), 0, extent[axis]) for axis in range(len(extent))]
    values = values.at[tuple(spot)].set(least)
    longest = extent.index(max(extent))
    spot[longest] = (spot[longest] + 1) % extent[longest]
    return values.at[tuple(spot)].set(top_value)


def setup_inputs(seed: int = 0, part: int = 0) -> dict:
    key_of = jax.random.split(jax.random.key(seed), 5)
    part_keys = jax.random.split(jax.random.fold_in(key_of[4], part), 5)
    queries = draw_queries(jax.random.fold_in(jax.random.fold_in(key_of[4], part), 71), part)
    latent_cache = draw_latent_cache(jax.random.fold_in(jax.random.fold_in(key_of[4], part), 71), part)
    block_picks = draw_block_picks(jax.random.fold_in(jax.random.fold_in(key_of[4], part), 71), part)
    lengths = plant(jax.random.randint(part_keys[3], (QROWS,), CONTEXT // 2, CONTEXT + 1), jax.random.fold_in(part_keys[3], 1), CONTEXT // 2, CONTEXT).astype(jnp.int32)
    return dict(queries=queries, latent_cache=latent_cache, block_picks=block_picks, lengths=lengths)


SOFTMAX_SCALE = 192.0 ** -0.5


def attend(query_rows, key_rows, positions, row_lengths):
    total_rows = query_rows.shape[0]
    step_rows = 512 if total_rows % 512 == 0 else total_rows
    block_count = total_rows // step_rows
    latent = key_rows[:, :LAT]

    def per_block(inputs):
        block_queries, block_lengths = inputs
        block_ratings = lax.dot_general(block_queries, key_rows, (((1,), (1,)), ((), ())), preferred_element_type=jnp.float32) * SOFTMAX_SCALE
        visible = positions[None, :] < block_lengths[:, None]
        row_max = jnp.max(jnp.where(visible, block_ratings, -jnp.inf), axis=1, keepdims=True)
        exponent = jnp.where(visible, jnp.exp(block_ratings - row_max), 0.0)
        normaliser = jnp.sum(exponent, axis=1, keepdims=True)
        weights = exponent.astype(jnp.bfloat16)
        result = jnp.dot(weights, latent, preferred_element_type=jnp.float32) / normaliser
        return result.astype(jnp.bfloat16)

    outputs = lax.map(per_block, (query_rows.reshape(block_count, step_rows, query_rows.shape[1]), row_lengths.reshape(block_count, step_rows)))
    return outputs.reshape(total_rows, LAT)


def reference(queries, latent_cache, block_picks, lengths):
    groups = block_picks.shape[0]
    per_group = queries.shape[0] // groups
    head_count = queries.shape[1]
    feature = queries.shape[2]
    within = jnp.arange(BLOCK, dtype=jnp.int32)

    def per_group_attend(group):
        chosen_blocks = lax.dynamic_index_in_dim(block_picks, group, 0, keepdims=False)
        positions = (chosen_blocks[:, None] * BLOCK + within[None, :]).reshape(-1).astype(jnp.int32)
        key_rows = jnp.take(latent_cache, positions, axis=0)
        first_row = (group * per_group).astype(jnp.int32)
        query_rows = lax.dynamic_slice_in_dim(queries, first_row, per_group, 0).reshape(per_group * head_count, feature)
        row_lengths = jnp.repeat(lax.dynamic_slice_in_dim(lengths, first_row, per_group, 0), head_count)
        return attend(query_rows, key_rows, positions, row_lengths)

    outputs = lax.map(per_group_attend, jnp.arange(groups, dtype=jnp.int32))
    return outputs.reshape(queries.shape[0], head_count, LAT)
```

```python
import functools

import jax
import jax.numpy as jnp
from jax import lax
from jax.experimental import pallas as pl
from jax.experimental.pallas import tpu as pltpu
from jax.sharding import PartitionSpec as P

LAT = 512
BLOCK = 64
TOPK = 32
LANES = 128

SOFTMAX_SCALE = 192.0 ** (-0.5)
LOG2E = 1.4426950408889634
MESH = pl.DeviceIdType.MESH
HIDDEN = -1e30


def gather_kernel(
    ctx_count, owned, units, picks_ref, flags_ref, cache_ref, keys_ref,
    all_flags, gath, flag_send, flag_recv, send, recv,
):
    feature = cache_ref.shape[2]
    rope = feature - LAT
    pair = 2 * BLOCK
    tall = pair * rope // LAT
    line = ctx_count // 4
    me = lax.axis_index("ctx")
    core = lax.rem(me, 2)
    y = lax.rem(me // 2, 2)
    z = me // 4

    def at(zz, yy, cc):
        return (zz * 2 + yy) * 2 + cc

    barrier = pltpu.get_barrier_semaphore()

    @pl.loop(1, ctx_count)
    def _(d):
        pl.semaphore_signal(
            barrier, inc=1, device_id={"ctx": lax.rem(me + d, ctx_count)}, device_id_type=MESH
        )

    pl.semaphore_wait(barrier, ctx_count - 1)

    def flag_copy(d):
        return pltpu.make_async_remote_copy(
            src_ref=flags_ref,
            dst_ref=all_flags.at[me],
            send_sem=flag_send.at[d],
            recv_sem=flag_recv.at[me],
            device_id={"ctx": lax.rem(me + d, ctx_count)},
            device_id_type=MESH,
        )

    def flag_arrival(source):
        return pltpu.make_async_remote_copy(
            src_ref=flags_ref,
            dst_ref=all_flags.at[source],
            send_sem=flag_send.at[0],
            recv_sem=flag_recv.at[source],
            device_id={"ctx": source},
            device_id_type=MESH,
        )

    @pl.loop(1, ctx_count)
    def _(d):
        flag_copy(d).start()

    all_flags[me] = flags_ref[...]

    @pl.loop(1, ctx_count)
    def _(d):
        flag_arrival(lax.rem(me + d, ctx_count)).wait_recv()

    named = jnp.minimum(jnp.max(all_flags[...], axis=0), 1)
    rows = named.shape[0]
    block_id = lax.broadcasted_iota(jnp.int32, (rows, LANES), 0) * LANES + lax.broadcasted_iota(
        jnp.int32, (rows, LANES), 1
    )
    mine = (named > 0) & (block_id // owned == me)

    def unit_copy(slot, local, way, target):
        return pltpu.make_async_remote_copy(
            src_ref=gath.at[slot],
            dst_ref=gath.at[slot],
            send_sem=send.at[local, way],
            recv_sem=recv.at[slot],
            device_id={"ctx": target},
            device_id_type=MESH,
        )

    def slot_of(zz, j):
        crossed = (j == units).astype(jnp.int32)
        yy = lax.rem(y + crossed, 2)
        u = j * (1 - crossed)
        return at(zz, yy, core) * units + u, (zz * 2 + yy) * units + u

    up = at(lax.rem(z + 1, line), y, core)
    down = at(lax.rem(z + line - 1, line), y, core)
    across = at(z, 1 - y, core)
    sibling = at(z, y, 1 - core)

    def sends(zz, j):
        valid = (zz >= 0) & (zz < line) & ((j < units) | (core == 1))
        own_line = j < units
        return (
            (0, up, valid & (zz <= z) & (z + 1 < line)),
            (1, down, valid & (zz >= z) & (z > 0)),
            (2, across, valid & own_line & ((zz == z) | (core == 0) | (j > 0))),
            (3, sibling, valid),
        )

    def forward(zz, j, skip=()):
        slot, local = slot_of(zz, j)
        for way, target, yes in sends(zz, j):
            if way not in skip:
                @pl.when(yes)
                def _():
                    unit_copy(slot, local, way, target).start()

    def arrived(slot):
        unit_copy(slot, 0, 0, sibling).wait_recv()

    past = ctx_count * owned
    last = jnp.int32(-1)
    for u in range(units):
        for h in range(2):
            last = jnp.min(jnp.where(mine & (block_id > last), block_id, past))
            tokens = cache_ref[jnp.minimum(last - me * owned, owned - 1)]
            gath[me * units + u, h * BLOCK : (h + 1) * BLOCK, :] = tokens[:, :LAT]
            tail = tokens[:, LAT:]
            parts = [tail[i * tall : (i + 1) * tall, :] for i in range(BLOCK // tall)]
            gath[me * units + u, pair:, h * (LAT // 2) : (h + 1) * (LAT // 2)] = jnp.concatenate(
                parts, axis=1
            )
        forward(z, jnp.int32(u))

    per = units + 1

    @pl.loop(0, per * (line - 1))
    def _(k):
        step = k // per
        j = lax.rem(k, per)
        for zz in (z + 1 + step, z - 1 - step):
            @pl.when((zz >= 0) & (zz < line) & ((j < units) | (core == 1)))
            def _():
                slot, _ = slot_of(zz, j)
                arrived(slot)
                forward(zz, j)

        @pl.when((k == 0) & (core == 1))
        def _():
            slot, _ = slot_of(z, jnp.int32(units))
            arrived(slot)
            forward(z, jnp.int32(units))

    @pl.loop(0, units * line)
    def _(k):
        zz = lax.rem(z + k // units, line)
        j = lax.rem(k, units)

        @pl.when((core == 0) | (j > 0))
        def _():
            slot = at(zz, 1 - y, core) * units + j
            local = (zz * 2 + 1 - y) * units + j
            arrived(slot)
            unit_copy(slot, local, 3, sibling).start()

    @pl.loop(0, 2 * line)
    def _(o):
        @pl.loop(0, units)
        def _(u):
            arrived((o * 2 + 1 - core) * units + u)

    for k in range(TOPK):
        p = picks_ref[0, k]
        owner = p // owned
        slot = jnp.sum(jnp.where((block_id // owned == owner) & (block_id < p), named, 0))
        unit = gath[owner * units + slot // 2]
        first = lax.rem(slot, 2) == 0
        keys_ref[k * BLOCK : (k + 1) * BLOCK, :LAT] = jnp.where(
            first, unit[:BLOCK], unit[BLOCK:pair]
        )
        tail = jnp.where(first, unit[pair:, : LAT // 2], unit[pair:, LAT // 2 :])
        keys_ref[k * BLOCK : (k + 1) * BLOCK, LAT:] = jnp.concatenate(
            [tail[:, i * rope : (i + 1) * rope] for i in range(BLOCK // tall)], axis=0
        )

    @pl.loop(1, ctx_count)
    def _(d):
        flag_copy(d).wait_send()

    @pl.loop(0, per * line)
    def _(k):
        zz = k // per
        j = lax.rem(k, per)
        slot, local = slot_of(zz, j)
        for way, target, yes in sends(zz, j):
            @pl.when(yes)
            def _():
                unit_copy(slot, local, way, target).wait_send()

    @pl.loop(0, units * line)
    def _(k):
        zz = k // units
        j = lax.rem(k, units)

        @pl.when((core == 0) | (j > 0))
        def _():
            slot = at(zz, 1 - y, core) * units + j
            local = (zz * 2 + 1 - y) * units + j
            unit_copy(slot, local, 3, sibling).wait_send()


def attend_kernel(per_step, lengths_ref, positions_ref, q_ref, keys_ref, out_ref):
    heads = q_ref.shape[1]
    feature = q_ref.shape[2]
    step = pl.program_id(0)
    q = q_ref[...].reshape(per_step * heads, feature)
    s = lax.dot_general(
        q, keys_ref[...], (((1,), (1,)), ((), ())), preferred_element_type=jnp.float32
    )
    for r in range(per_step):
        visible = positions_ref[...] < lengths_ref[step * per_step + r]
        part = jnp.where(visible, s[r * heads : (r + 1) * heads, :], HIDDEN)
        top = jnp.max(part, axis=1, keepdims=True)
        e = jnp.exp2((part - top) * (SOFTMAX_SCALE * LOG2E))
        total = jnp.sum(e, axis=1, keepdims=True)
        o = jnp.dot(
            e.astype(jnp.bfloat16), keys_ref[:, :LAT], preferred_element_type=jnp.float32
        )
        out_ref[r] = (o / total).astype(jnp.bfloat16)


def shards(queries, latent_cache, block_picks, lengths):
    ctx_count = lax.axis_size("ctx")
    feature = latent_cache.shape[1]
    owned = latent_cache.shape[0] // BLOCK
    units = max(1, 2 * TOPK // ctx_count)
    own_picks = block_picks[0]
    total = ctx_count * owned
    flags = jnp.sum(
        (own_picks[:, None] == jnp.arange(total, dtype=jnp.int32)[None, :]).astype(jnp.int32),
        axis=0,
    ).reshape(total // LANES, LANES)
    flags = jnp.pad(flags, ((0, -flags.shape[0] % 8), (0, 0)))
    within = jnp.arange(BLOCK, dtype=jnp.int32)
    positions = (own_picks[:, None] * BLOCK + within[None, :]).reshape(1, -1)
    tall = 2 * BLOCK + 2 * BLOCK * (feature - LAT) // LAT
    keys = pl.pallas_call(
        functools.partial(gather_kernel, ctx_count, owned, units),
        out_shape=jax.ShapeDtypeStruct((TOPK * BLOCK, feature), jnp.bfloat16),
        in_specs=[
            pl.BlockSpec(memory_space=pltpu.SMEM),
            pl.BlockSpec(memory_space=pltpu.VMEM),
            pl.BlockSpec(memory_space=pltpu.VMEM),
        ],
        out_specs=pl.BlockSpec(memory_space=pltpu.VMEM),
        scratch_shapes=[
            pltpu.VMEM((ctx_count,) + flags.shape, jnp.int32),
            pltpu.VMEM((ctx_count * units, tall, LAT), jnp.bfloat16),
            pltpu.SemaphoreType.DMA((ctx_count,)),
            pltpu.SemaphoreType.DMA((ctx_count,)),
            pltpu.SemaphoreType.DMA((ctx_count // 2 * units, 4)),
            pltpu.SemaphoreType.DMA((ctx_count * units,)),
        ],
        compiler_params=pltpu.CompilerParams(
            collective_id=0, has_side_effects=True, vmem_limit_bytes=40 * 1024 * 1024
        ),
    )(block_picks, flags, latent_cache.reshape(owned, BLOCK, feature))
    rows, heads, _ = queries.shape
    per_step = 2 if rows % 2 == 0 else 1
    return pl.pallas_call(
        functools.partial(attend_kernel, per_step),
        grid=(rows // per_step,),
        out_shape=jax.ShapeDtypeStruct((rows, heads, LAT), jnp.bfloat16),
        in_specs=[
            pl.BlockSpec(memory_space=pltpu.SMEM),
            pl.BlockSpec(memory_space=pltpu.VMEM),
            pl.BlockSpec((per_step, heads, feature), lambda i: (i, 0, 0)),
            pl.BlockSpec((TOPK * BLOCK, feature), lambda i: (0, 0)),
        ],
        out_specs=pl.BlockSpec((per_step, heads, LAT), lambda i: (i, 0, 0)),
        compiler_params=pltpu.CompilerParams(vmem_limit_bytes=40 * 1024 * 1024),
    )(lengths, positions, queries, keys)


def solution(mesh):
    placed = (
        P(("groups", "ctx"), None, None),
        P(("groups", "ctx"), None),
        P(("groups", "ctx"), None),
        P(("groups", "ctx")),
    )
    return jax.shard_map(
        shards,
        mesh=mesh,
        in_specs=placed,
        out_specs=P(("groups", "ctx"), None, None),
        check_vma=False,
    )
```

```python
import functools

import jax
import jax.numpy as jnp
from jax import lax
from jax.experimental import pallas as pl
from jax.experimental.pallas import tpu as pltpu
from jax.sharding import PartitionSpec as P

LAT = 512
BLOCK = 64
TOPK = 32
LANES = 128

SOFTMAX_SCALE = 192.0 ** (-0.5)
LOG2E = 1.4426950408889634
MESH = pl.DeviceIdType.MESH
HIDDEN = -1e30


def step_kernel(
    ctx_count, owned, units, picks_ref, lengths_ref, queries_ref, cache_ref, out_ref,
    raw_q, q_ref, flags_ref, all_flags, gath, pool, keys_t, values, positions, order,
    top_ref, total_ref, acc_ref, q_sem, flag_send, flag_recv, send, recv,
):
    rows, feature, heads = queries_ref.shape
    rope = feature - LAT
    pair = 2 * BLOCK
    tall = pair * rope // LAT
    line = ctx_count // 4
    late_blocks = 2 * units
    early_blocks = TOPK - late_blocks
    me = lax.axis_index("ctx")
    core = lax.rem(me, 2)
    y = lax.rem(me // 2, 2)
    z = me // 4
    far = jnp.where(2 * z < line, line - 1, 0)

    fetch = pltpu.make_async_copy(queries_ref, raw_q, q_sem)
    fetch.start()

    def at(zz, yy, cc):
        return (zz * 2 + yy) * 2 + cc

    barrier = pltpu.get_barrier_semaphore()

    @pl.loop(1, ctx_count)
    def _(d):
        pl.semaphore_signal(
            barrier, inc=1, device_id={"ctx": lax.rem(me + d, ctx_count)}, device_id_type=MESH
        )

    flag_rows = flags_ref.shape[0]
    block_id = lax.broadcasted_iota(jnp.int32, (flag_rows, LANES), 0) * LANES
    block_id += lax.broadcasted_iota(jnp.int32, (flag_rows, LANES), 1)
    lane = lax.broadcasted_iota(jnp.int32, (1, LANES), 1)
    flags = jnp.zeros((flag_rows, LANES), jnp.int32)
    ordered = jnp.zeros((1, LANES), jnp.int32)
    early_seen = jnp.int32(0)
    for k in range(TOPK):
        p = picks_ref[0, k]
        owner = p // owned
        is_late = (owner // 4 == far) & (lax.rem(owner // 2, 2) != y)
        place = jnp.where(is_late, TOPK - 1 - (k - early_seen), early_seen)
        early_seen += jnp.where(is_late, 0, 1)
        flags = jnp.where(block_id == p, 1, flags)
        ordered = jnp.where(lane == place, p, ordered)
    flags_ref[...] = flags

    pl.semaphore_wait(barrier, ctx_count - 1)

    def flag_copy(d):
        return pltpu.make_async_remote_copy(
            src_ref=flags_ref,
            dst_ref=all_flags.at[me],
            send_sem=flag_send.at[d],
            recv_sem=flag_recv.at[me],
            device_id={"ctx": lax.rem(me + d, ctx_count)},
            device_id_type=MESH,
        )

    def flag_arrival(source):
        return pltpu.make_async_remote_copy(
            src_ref=flags_ref,
            dst_ref=all_flags.at[source],
            send_sem=flag_send.at[0],
            recv_sem=flag_recv.at[source],
            device_id={"ctx": source},
            device_id_type=MESH,
        )

    @pl.loop(1, ctx_count)
    def _(d):
        flag_copy(d).start()

    all_flags[me] = flags

    @pl.loop(1, ctx_count)
    def _(d):
        flag_arrival(lax.rem(me + d, ctx_count)).wait_recv()

    named = jnp.minimum(jnp.max(all_flags[...], axis=0), 1)
    mine = (named > 0) & (block_id // owned == me)

    def unit_copy(slot, local, way, target):
        return pltpu.make_async_remote_copy(
            src_ref=gath.at[slot],
            dst_ref=gath.at[slot],
            send_sem=send.at[local, way],
            recv_sem=recv.at[slot],
            device_id={"ctx": target},
            device_id_type=MESH,
        )

    def slot_of(zz, j):
        crossed = (j == units).astype(jnp.int32)
        yy = lax.rem(y + crossed, 2)
        u = j * (1 - crossed)
        return at(zz, yy, core) * units + u, (zz * 2 + yy) * units + u

    up = at(lax.rem(z + 1, line), y, core)
    down = at(lax.rem(z + line - 1, line), y, core)
    across = at(z, 1 - y, core)
    sibling = at(z, y, 1 - core)

    def sends(zz, j):
        valid = (zz >= 0) & (zz < line) & ((j < units) | (core == 1))
        own_line = j < units
        return (
            (0, up, valid & (zz <= z) & (z + 1 < line)),
            (1, down, valid & (zz >= z) & (z > 0)),
            (2, across, valid & own_line & ((zz == z) | (core == 0) | (j > 0))),
            (3, sibling, valid),
        )

    def forward(zz, j, skip=()):
        slot, local = slot_of(zz, j)
        for way, target, yes in sends(zz, j):
            if way not in skip:
                @pl.when(yes)
                def _():
                    unit_copy(slot, local, way, target).start()

    def arrived(slot):
        unit_copy(slot, 0, 0, sibling).wait_recv()

    past = ctx_count * owned
    last = jnp.int32(-1)
    token = lax.broadcasted_iota(jnp.int32, (pair, owned * BLOCK), 0)
    column = lax.broadcasted_iota(jnp.int32, (pair, owned * BLOCK), 1)
    for u in range(units):
        starts = []
        for h in range(2):
            last = jnp.min(jnp.where(mine & (block_id > last), block_id, past))
            starts.append(jnp.minimum(last - me * owned, owned - 1) * BLOCK)
        wanted = jnp.where(token < BLOCK, starts[0] + token, starts[1] + token - BLOCK)
        chosen = jnp.where(column == wanted, 1.0, 0.0).astype(jnp.bfloat16)
        tokens = lax.dot_general(
            chosen, cache_ref[...], (((1,), (1,)), ((), ())), preferred_element_type=jnp.float32
        ).astype(jnp.bfloat16)
        tail = tokens[:, LAT:]
        packed = jnp.concatenate(
            [tail[i * tall : (i + 1) * tall, :] for i in range(pair // tall)], axis=1
        )
        gath[me * units + u, :pair, :] = tokens[:, :LAT]
        gath[me * units + u, pair:, :] = packed
        pool[me * units + u, :pair, :] = tokens[:, :LAT]
        pool[me * units + u, pair:, :] = packed
        forward(z, jnp.int32(u))

    def keep(slot):
        pool[slot] = gath[slot]

    fetch.wait()

    def turn(row):
        q_ref[row] = raw_q[row].T

    for k in range(TOPK):
        order[k] = jnp.sum(jnp.where(lane == k, ordered, 0))

    per = units + 1

    @pl.loop(0, per * (line - 1))
    def _(k):
        step = k // per
        j = lax.rem(k, per)
        for zz in (z + 1 + step, z - 1 - step):
            @pl.when((zz >= 0) & (zz < line) & ((j < units) | (core == 1)))
            def _():
                slot, _ = slot_of(zz, j)
                arrived(slot)
                forward(zz, j)
                keep(slot)

        @pl.when((k == 0) & (core == 1))
        def _():
            slot, _ = slot_of(z, jnp.int32(units))
            arrived(slot)
            forward(z, jnp.int32(units))
            keep(slot)

        @pl.when(k < rows)
        def _():
            turn(lax.rem(k, rows))

    @pl.loop(min(rows, per * (line - 1)), rows)
    def _(row):
        turn(row)

    def cross(zz, j):
        @pl.when((core == 0) | (j > 0))
        def _():
            slot = at(zz, 1 - y, core) * units + j
            local = (zz * 2 + 1 - y) * units + j
            arrived(slot)
            unit_copy(slot, local, 3, sibling).start()
            keep(slot)

    def beside(owner, u):
        slot = owner * units + u
        arrived(slot)
        keep(slot)

    @pl.loop(0, units * line)
    def _(k):
        zz = lax.rem(z + k // units, line)

        @pl.when(zz != far)
        def _():
            cross(zz, lax.rem(k, units))

    @pl.loop(0, line * 2 * units)
    def _(k):
        o = k // units

        @pl.when((o // 2 != far) | (lax.rem(o, 2) == y))
        def _():
            beside(o * 2 + 1 - core, lax.rem(k, units))

    def fill(first_block, blocks):
        for k in range(first_block, first_block + blocks, 2):
            latent, tails, places = [], [], []
            for h in range(2):
                p = order[k + h]
                owner = p // owned
                slot = jnp.sum(jnp.where((block_id // owned == owner) & (block_id < p), named, 0))
                unit = pool[owner * units + slot // 2]
                first = lax.rem(slot, 2) == 0
                latent.append(jnp.where(first, unit[:BLOCK], unit[BLOCK:pair]))
                tail = jnp.where(first, unit[pair:, : LAT // 2], unit[pair:, LAT // 2 :])
                tails += [tail[:, i * rope : (i + 1) * rope] for i in range(BLOCK // tall)]
                places.append(p * BLOCK)
            latent = jnp.concatenate(latent, axis=0)
            tails = jnp.concatenate(tails, axis=0)
            span = slice(k * BLOCK, (k + 2) * BLOCK)
            values[span, :] = latent
            keys_t[:LAT, span] = latent.T
            keys_t[LAT:, span] = tails.T
            positions[:, span] = jnp.where(lane < BLOCK, places[0] + lane, places[1] + lane - BLOCK)

    scale = SOFTMAX_SCALE * LOG2E
    pairs = rows // 2

    def scores(i, span):
        q = q_ref[pl.ds(2 * i, 2)].reshape(2 * heads, feature)
        s = jnp.dot(q, keys_t[:, span], preferred_element_type=jnp.float32)
        where = positions[:, span]
        return jnp.concatenate(
            [
                jnp.where(where < lengths_ref[2 * i + r], s[r * heads : (r + 1) * heads], HIDDEN)
                for r in range(2)
            ],
            axis=0,
        )

    early = slice(0, early_blocks * BLOCK)
    late = slice(early_blocks * BLOCK, TOPK * BLOCK)
    fill(0, early_blocks)

    @pl.loop(0, pairs)
    def _(i):
        s = scores(i, early)
        top = jnp.max(s, axis=1, keepdims=True)
        e = jnp.exp2((s - top) * scale)
        top_ref[i] = top
        total_ref[i] = jnp.sum(e, axis=1, keepdims=True)
        acc_ref[i] = jnp.dot(
            e.astype(jnp.bfloat16), values[early, :], preferred_element_type=jnp.float32
        )

        @pl.when(lax.rem(i, 2) == 1)
        def _():
            @pl.when(i // 2 < units)
            def _():
                cross(far, i // 2)

    @pl.loop(min(units, pairs // 2), units)
    def _(u):
        cross(far, u)

    @pl.loop(0, units)
    def _(u):
        beside(at(far, 1 - y, 1 - core), u)

    fill(early_blocks, late_blocks)

    @pl.loop(0, pairs)
    def _(i):
        s = scores(i, late)
        before = top_ref[i]
        top = jnp.maximum(before, jnp.max(s, axis=1, keepdims=True))
        e = jnp.exp2((s - top) * scale)
        shrink = jnp.exp2((before - top) * scale)
        total = total_ref[i] * shrink + jnp.sum(e, axis=1, keepdims=True)
        o = acc_ref[i] * shrink + jnp.dot(
            e.astype(jnp.bfloat16), values[late, :], preferred_element_type=jnp.float32
        )
        out_ref[pl.ds(2 * i, 2)] = (o / total).astype(jnp.bfloat16).reshape(2, heads, LAT)

    @pl.loop(1, ctx_count)
    def _(d):
        flag_copy(d).wait_send()

    @pl.loop(0, per * line)
    def _(k):
        zz = k // per
        j = lax.rem(k, per)
        slot, local = slot_of(zz, j)
        for way, target, yes in sends(zz, j):
            @pl.when(yes)
            def _():
                unit_copy(slot, local, way, target).wait_send()

    @pl.loop(0, units * line)
    def _(k):
        zz = k // units
        j = lax.rem(k, units)

        @pl.when((core == 0) | (j > 0))
        def _():
            slot = at(zz, 1 - y, core) * units + j
            local = (zz * 2 + 1 - y) * units + j
            unit_copy(slot, local, 3, sibling).wait_send()


def shards(queries, latent_cache, block_picks, lengths):
    ctx_count = lax.axis_size("ctx")
    rows, heads, feature = queries.shape
    owned = latent_cache.shape[0] // BLOCK
    units = max(1, 2 * TOPK // ctx_count)
    flag_rows = -(-(ctx_count * owned) // LANES // 8) * 8
    tall = 2 * BLOCK + 2 * BLOCK * (feature - LAT) // LAT
    keys = TOPK * BLOCK
    return pl.pallas_call(
        functools.partial(step_kernel, ctx_count, owned, units),
        out_shape=jax.ShapeDtypeStruct((rows, heads, LAT), jnp.bfloat16),
        in_specs=[
            pl.BlockSpec(memory_space=pltpu.SMEM),
            pl.BlockSpec(memory_space=pltpu.SMEM),
            pl.BlockSpec(memory_space=pl.ANY),
            pl.BlockSpec(memory_space=pltpu.VMEM),
        ],
        out_specs=pl.BlockSpec(memory_space=pltpu.VMEM),
        scratch_shapes=[
            pltpu.VMEM((rows, feature, heads), jnp.bfloat16),
            pltpu.VMEM((rows, heads, feature), jnp.bfloat16),
            pltpu.VMEM((flag_rows, LANES), jnp.int32),
            pltpu.VMEM((ctx_count, flag_rows, LANES), jnp.int32),
            pltpu.VMEM((ctx_count * units, tall, LAT), jnp.bfloat16),
            pltpu.VMEM((ctx_count * units, tall, LAT), jnp.bfloat16),
            pltpu.VMEM((feature, keys), jnp.bfloat16),
            pltpu.VMEM((keys, LAT), jnp.bfloat16),
            pltpu.VMEM((1, keys), jnp.int32),
            pltpu.SMEM((TOPK,), jnp.int32),
            pltpu.VMEM((rows // 2, 2 * heads, 1), jnp.float32),
            pltpu.VMEM((rows // 2, 2 * heads, 1), jnp.float32),
            pltpu.VMEM((rows // 2, 2 * heads, LAT), jnp.float32),
            pltpu.SemaphoreType.DMA,
            pltpu.SemaphoreType.DMA((ctx_count,)),
            pltpu.SemaphoreType.DMA((ctx_count,)),
            pltpu.SemaphoreType.DMA((ctx_count // 2 * units, 4)),
            pltpu.SemaphoreType.DMA((ctx_count * units,)),
        ],
        compiler_params=pltpu.CompilerParams(
            collective_id=0, has_side_effects=True, vmem_limit_bytes=60 * 1024 * 1024
        ),
    )(block_picks, lengths, jnp.swapaxes(queries, 1, 2), latent_cache.T)


def solution(mesh):
    placed = (
        P(("groups", "ctx"), None, None),
        P(("groups", "ctx"), None),
        P(("groups", "ctx"), None),
        P(("groups", "ctx")),
    )
    return jax.shard_map(
        shards,
        mesh=mesh,
        in_specs=placed,
        out_specs=P(("groups", "ctx"), None, None),
        check_vma=False,
    )
```

```python
import functools

import jax
import jax.numpy as jnp
from jax import lax
from jax.experimental import pallas as pl
from jax.experimental.pallas import tpu as pltpu
from jax.sharding import PartitionSpec as P

LAT = 512
BLOCK = 64
TOPK = 32
LANES = 128

SOFTMAX_SCALE = 192.0 ** (-0.5)
LOG2E = 1.4426950408889634
MESH = pl.DeviceIdType.MESH
HIDDEN = -1e30


def step_kernel(
    ctx_count, owned, units, picks_ref, lengths_ref, queries_ref, cache_ref, out_ref,
    raw_q, near_cache, q_ref, flags_ref, all_flags, gath, pool, keys_t, values, positions, order,
    top_ref, total_ref, acc_ref, q_sem, cache_sem, flag_send, flag_recv, send, recv,
):
    rows, feature, heads = queries_ref.shape
    rope = feature - LAT
    pair = 2 * BLOCK
    tall = pair * rope // LAT
    line = ctx_count // 4
    late_blocks = 4 * units
    early_blocks = TOPK - late_blocks
    me = lax.axis_index("ctx")
    core = lax.rem(me, 2)
    y = lax.rem(me // 2, 2)
    z = me // 4
    far = jnp.where(2 * z < line, line - 1, 0)

    fetch = pltpu.make_async_copy(queries_ref, raw_q, q_sem)
    fetch_cache = pltpu.make_async_copy(cache_ref, near_cache, cache_sem)
    fetch_cache.start()
    fetch.start()

    def at(zz, yy, cc):
        return (zz * 2 + yy) * 2 + cc

    barrier = pltpu.get_barrier_semaphore()

    @pl.loop(1, ctx_count)
    def _(d):
        pl.semaphore_signal(
            barrier, inc=1, device_id={"ctx": lax.rem(me + d, ctx_count)}, device_id_type=MESH
        )

    flag_rows = flags_ref.shape[0]
    block_id = lax.broadcasted_iota(jnp.int32, (flag_rows, LANES), 0) * LANES
    block_id += lax.broadcasted_iota(jnp.int32, (flag_rows, LANES), 1)
    lane = lax.broadcasted_iota(jnp.int32, (1, LANES), 1)
    flags = jnp.zeros((flag_rows, LANES), jnp.int32)
    ordered = jnp.zeros((1, LANES), jnp.int32)
    early_seen = jnp.int32(0)
    for k in range(TOPK):
        p = picks_ref[0, k]
        owner = p // owned
        is_late = owner // 4 == far
        place = jnp.where(is_late, TOPK - 1 - (k - early_seen), early_seen)
        early_seen += jnp.where(is_late, 0, 1)
        flags = jnp.where(block_id == p, 1, flags)
        ordered = jnp.where(lane == place, p, ordered)
    flags_ref[...] = flags

    pl.semaphore_wait(barrier, ctx_count - 1)

    def flag_copy(d):
        return pltpu.make_async_remote_copy(
            src_ref=flags_ref,
            dst_ref=all_flags.at[me],
            send_sem=flag_send.at[d],
            recv_sem=flag_recv.at[me],
            device_id={"ctx": lax.rem(me + d, ctx_count)},
            device_id_type=MESH,
        )

    def flag_arrival(source):
        return pltpu.make_async_remote_copy(
            src_ref=flags_ref,
            dst_ref=all_flags.at[source],
            send_sem=flag_send.at[0],
            recv_sem=flag_recv.at[source],
            device_id={"ctx": source},
            device_id_type=MESH,
        )

    @pl.loop(1, ctx_count)
    def _(d):
        flag_copy(d).start()

    all_flags[me] = flags

    @pl.loop(1, ctx_count)
    def _(d):
        flag_arrival(lax.rem(me + d, ctx_count)).wait_recv()

    named = jnp.minimum(jnp.max(all_flags[...], axis=0), 1)
    mine = (named > 0) & (block_id // owned == me)

    def unit_copy(slot, local, way, target):
        return pltpu.make_async_remote_copy(
            src_ref=gath.at[slot],
            dst_ref=gath.at[slot],
            send_sem=send.at[local, way],
            recv_sem=recv.at[slot],
            device_id={"ctx": target},
            device_id_type=MESH,
        )

    def slot_of(zz, j):
        crossed = (j == units).astype(jnp.int32)
        yy = lax.rem(y + crossed, 2)
        u = j * (1 - crossed)
        return at(zz, yy, core) * units + u, (zz * 2 + yy) * units + u

    up = at(lax.rem(z + 1, line), y, core)
    down = at(lax.rem(z + line - 1, line), y, core)
    across = at(z, 1 - y, core)
    sibling = at(z, y, 1 - core)

    def sends(zz, j):
        valid = (zz >= 0) & (zz < line) & ((j < units) | (core == 1))
        own_line = j < units
        return (
            (0, up, valid & (zz <= z) & (z + 1 < line)),
            (1, down, valid & (zz >= z) & (z > 0)),
            (2, across, valid & own_line & ((zz == z) | (core == 0) | (j > 0))),
            (3, sibling, valid),
        )

    def forward(zz, j, skip=()):
        slot, local = slot_of(zz, j)
        for way, target, yes in sends(zz, j):
            if way not in skip:
                @pl.when(yes)
                def _():
                    unit_copy(slot, local, way, target).start()

    def arrived(slot):
        unit_copy(slot, 0, 0, sibling).wait_recv()

    past = ctx_count * owned
    fetch_cache.wait()
    last = jnp.int32(-1)
    token = lax.broadcasted_iota(jnp.int32, (pair, owned * BLOCK), 0)
    column = lax.broadcasted_iota(jnp.int32, (pair, owned * BLOCK), 1)
    for u in range(units):
        starts = []
        for h in range(2):
            last = jnp.min(jnp.where(mine & (block_id > last), block_id, past))
            starts.append(jnp.minimum(last - me * owned, owned - 1) * BLOCK)
        wanted = jnp.where(token < BLOCK, starts[0] + token, starts[1] + token - BLOCK)
        chosen = jnp.where(column == wanted, 1.0, 0.0).astype(jnp.bfloat16)
        tokens = lax.dot_general(
            chosen, near_cache[...], (((1,), (1,)), ((), ())), preferred_element_type=jnp.float32
        ).astype(jnp.bfloat16)
        tail = tokens[:, LAT:]
        packed = jnp.concatenate(
            [tail[i * tall : (i + 1) * tall, :] for i in range(pair // tall)], axis=1
        )
        gath[me * units + u, :pair, :] = tokens[:, :LAT]
        gath[me * units + u, pair:, :] = packed
        pool[me * units + u, :pair, :] = tokens[:, :LAT]
        pool[me * units + u, pair:, :] = packed
        forward(z, jnp.int32(u))

    def keep(slot):
        pool[slot] = gath[slot]

    fetch.wait()

    def turn(row):
        q_ref[row] = raw_q[row].T

    for k in range(TOPK):
        order[k] = jnp.sum(jnp.where(lane == k, ordered, 0))

    per = units + 1

    def along(k):
        step = k // per
        j = lax.rem(k, per)
        for zz in (z + 1 + step, z - 1 - step):
            @pl.when((zz >= 0) & (zz < line) & ((j < units) | (core == 1)))
            def _():
                slot, _ = slot_of(zz, j)
                arrived(slot)
                forward(zz, j)
                keep(slot)

    main = per * (line - 2)

    @pl.loop(0, main)
    def _(k):
        along(k)

        @pl.when((k == 0) & (core == 1))
        def _():
            slot, _ = slot_of(z, jnp.int32(units))
            arrived(slot)
            forward(z, jnp.int32(units))
            keep(slot)

        @pl.when(k < rows)
        def _():
            turn(lax.rem(k, rows))

    @pl.loop(min(rows, main), rows)
    def _(row):
        turn(row)

    def cross(zz, j):
        @pl.when((core == 0) | (j > 0))
        def _():
            slot = at(zz, 1 - y, core) * units + j
            local = (zz * 2 + 1 - y) * units + j
            arrived(slot)
            unit_copy(slot, local, 3, sibling).start()
            keep(slot)

    def beside(owner, u):
        slot = owner * units + u
        arrived(slot)
        keep(slot)

    @pl.loop(0, units * line)
    def _(k):
        zz = lax.rem(z + k // units, line)

        @pl.when(k // units == line - 2)
        def _():
            along(main + lax.rem(k, units))

        @pl.when(zz != far)
        def _():
            cross(zz, lax.rem(k, units))

    @pl.loop(0, line * 2 * units)
    def _(k):
        o = k // units

        @pl.when(o // 2 != far)
        def _():
            beside(o * 2 + 1 - core, lax.rem(k, units))

    def fill(first_block, blocks):
        for k in range(first_block, first_block + blocks, 2):
            latent, tails, places = [], [], []
            for h in range(2):
                p = order[k + h]
                owner = p // owned
                slot = jnp.sum(jnp.where((block_id // owned == owner) & (block_id < p), named, 0))
                unit = pool[owner * units + slot // 2]
                first = lax.rem(slot, 2) == 0
                latent.append(jnp.where(first, unit[:BLOCK], unit[BLOCK:pair]))
                tail = jnp.where(first, unit[pair:, : LAT // 2], unit[pair:, LAT // 2 :])
                tails += [tail[:, i * rope : (i + 1) * rope] for i in range(BLOCK // tall)]
                places.append(p * BLOCK)
            latent = jnp.concatenate(latent, axis=0)
            tails = jnp.concatenate(tails, axis=0)
            span = slice(k * BLOCK, (k + 2) * BLOCK)
            values[span, :] = latent
            keys_t[:LAT, span] = latent.T
            keys_t[LAT:, span] = tails.T
            positions[:, span] = jnp.where(lane < BLOCK, places[0] + lane, places[1] + lane - BLOCK)

    scale = SOFTMAX_SCALE * LOG2E
    merged = 2 if rows % 4 == 0 else 1
    groups = rows // 2 // merged

    def scores(i, span):
        q = q_ref[pl.ds(2 * i, 2)].reshape(2 * heads, feature)
        s = jnp.dot(q, keys_t[:, span], preferred_element_type=jnp.float32)
        where = positions[:, span]
        return jnp.concatenate(
            [
                jnp.where(where < lengths_ref[2 * i + r], s[r * heads : (r + 1) * heads], HIDDEN)
                for r in range(2)
            ],
            axis=0,
        )

    early = slice(0, early_blocks * BLOCK)
    late = slice(early_blocks * BLOCK, TOPK * BLOCK)
    fill(0, early_blocks)

    @pl.loop(0, groups)
    def _(g):
        for m in range(merged):
            i = g * merged + m
            s = scores(i, early)
            top = jnp.max(s, axis=1, keepdims=True)
            e = jnp.exp2((s - top) * scale)
            top_ref[i] = top
            total_ref[i] = jnp.sum(e, axis=1, keepdims=True)
            acc_ref[i] = jnp.dot(
                e.astype(jnp.bfloat16), values[early, :], preferred_element_type=jnp.float32
            )

        @pl.when(g < units)
        def _():
            cross(far, g)

    @pl.loop(min(units, groups), units)
    def _(u):
        cross(far, u)

    along(jnp.int32(main + units))

    @pl.loop(0, 2 * units)
    def _(k):
        beside(at(far, k // units, 1 - core), lax.rem(k, units))

    fill(early_blocks, late_blocks)

    @pl.loop(0, groups)
    def _(g):
        for m in range(merged):
            i = g * merged + m
            s = scores(i, late)
            before = top_ref[i]
            top = jnp.maximum(before, jnp.max(s, axis=1, keepdims=True))
            e = jnp.exp2((s - top) * scale)
            shrink = jnp.exp2((before - top) * scale)
            total = total_ref[i] * shrink + jnp.sum(e, axis=1, keepdims=True)
            o = acc_ref[i] * shrink + jnp.dot(
                e.astype(jnp.bfloat16), values[late, :], preferred_element_type=jnp.float32
            )
            out_ref[pl.ds(2 * i, 2)] = (o / total).astype(jnp.bfloat16).reshape(2, heads, LAT)

    @pl.loop(1, ctx_count)
    def _(d):
        flag_copy(d).wait_send()

    @pl.loop(0, per * line)
    def _(k):
        zz = k // per
        j = lax.rem(k, per)
        slot, local = slot_of(zz, j)
        for way, target, yes in sends(zz, j):
            @pl.when(yes)
            def _():
                unit_copy(slot, local, way, target).wait_send()

    @pl.loop(0, units * line)
    def _(k):
        zz = k // units
        j = lax.rem(k, units)

        @pl.when((core == 0) | (j > 0))
        def _():
            slot = at(zz, 1 - y, core) * units + j
            local = (zz * 2 + 1 - y) * units + j
            unit_copy(slot, local, 3, sibling).wait_send()


def shards(queries, latent_cache, block_picks, lengths):
    ctx_count = lax.axis_size("ctx")
    rows, heads, feature = queries.shape
    owned = latent_cache.shape[0] // BLOCK
    units = max(1, 2 * TOPK // ctx_count)
    flag_rows = -(-(ctx_count * owned) // LANES // 8) * 8
    tall = 2 * BLOCK + 2 * BLOCK * (feature - LAT) // LAT
    keys = TOPK * BLOCK
    return pl.pallas_call(
        functools.partial(step_kernel, ctx_count, owned, units),
        out_shape=jax.ShapeDtypeStruct((rows, heads, LAT), jnp.bfloat16),
        in_specs=[
            pl.BlockSpec(memory_space=pltpu.SMEM),
            pl.BlockSpec(memory_space=pltpu.SMEM),
            pl.BlockSpec(memory_space=pl.ANY),
            pl.BlockSpec(memory_space=pl.ANY),
        ],
        out_specs=pl.BlockSpec(memory_space=pltpu.VMEM),
        scratch_shapes=[
            pltpu.VMEM((rows, feature, heads), jnp.bfloat16),
            pltpu.VMEM((feature, owned * BLOCK), jnp.bfloat16),
            pltpu.VMEM((rows, heads, feature), jnp.bfloat16),
            pltpu.VMEM((flag_rows, LANES), jnp.int32),
            pltpu.VMEM((ctx_count, flag_rows, LANES), jnp.int32),
            pltpu.VMEM((ctx_count * units, tall, LAT), jnp.bfloat16),
            pltpu.VMEM((ctx_count * units, tall, LAT), jnp.bfloat16),
            pltpu.VMEM((feature, keys), jnp.bfloat16),
            pltpu.VMEM((keys, LAT), jnp.bfloat16),
            pltpu.VMEM((1, keys), jnp.int32),
            pltpu.SMEM((TOPK,), jnp.int32),
            pltpu.VMEM((rows // 2, 2 * heads, 1), jnp.float32),
            pltpu.VMEM((rows // 2, 2 * heads, 1), jnp.float32),
            pltpu.VMEM((rows // 2, 2 * heads, LAT), jnp.float32),
            pltpu.SemaphoreType.DMA,
            pltpu.SemaphoreType.DMA,
            pltpu.SemaphoreType.DMA((ctx_count,)),
            pltpu.SemaphoreType.DMA((ctx_count,)),
            pltpu.SemaphoreType.DMA((ctx_count // 2 * units, 4)),
            pltpu.SemaphoreType.DMA((ctx_count * units,)),
        ],
        compiler_params=pltpu.CompilerParams(
            collective_id=0, has_side_effects=True, vmem_limit_bytes=60 * 1024 * 1024
        ),
    )(block_picks, lengths, jnp.swapaxes(queries, 1, 2), latent_cache.T)


def solution(mesh):
    placed = (
        P(("groups", "ctx"), None, None),
        P(("groups", "ctx"), None),
        P(("groups", "ctx"), None),
        P(("groups", "ctx")),
    )
    return jax.shard_map(
        shards,
        mesh=mesh,
        in_specs=placed,
        out_specs=P(("groups", "ctx"), None, None),
        check_vma=False,
    )
```
